256 devices in a mesh: rows: 64 (over z, x, core), cols: 4 (over y).
Axes of the slice: x: 4, y: 4, z: 8, core: 2. Of those that a mesh axis runs over, the one named last changes fastest.
Arguments:
- tables: float32 [4, 32768, 512], P(None, 'rows', 'cols'), may hold values from -1.5 to 1.5
- dense_features: float32 [2048, 512], P('rows', 'cols'), may hold values from -6 to 6
- slot_rows: int32 [64, 64, 4, 64], P('rows'), may hold values from 0 to 511, as said below
- slot_examples: int32 [64, 64, 4, 64], P('rows'), may hold values from 0 to 31, as said below
- slot_counts: int32 [64, 64, 4], P('rows'), may hold values from 21 to 64, as said below
Outputs:
- pooled: float32 [2048, 4, 512], P('rows', None, 'cols')
- interactions: float32 [2048, 10], P('rows')
The draws below stay inside these ranges and needn't reach their ends.
Inputs may be any that keep to these rules, and one draw needn't show every extreme that they name: slot_rows[s, o, t, c] names row o * 512 + value of table t. `slot_examples`: an example of the source device s. `slot_counts`: slots 0 to count - 1 of a bucket are live, the others unused; some bucket of every draw is full.
All inputs are finite; a program needn't handle non-finite values.
Results may differ from the reference program's by a relative error of at most 0.0003.
Values sent between devices are 32-bit elements; how exact they have to be, the bound alone decides.
A program may use at most 64 MiB of HBM per device.

```python
import jax
import jax.numpy as jnp
import numpy as np
from jax import lax

E = 512
TABLES = 4
ROWS_DEV = 512
B_DEV = 32
CAP = 64
BATCH = 2048
TABLE_ROWS = 32768
N_ROWS = 64


def draw_slot_counts(key, part):
    first_key, second_key = jax.random.split(jax.random.fold_in(key, 11))
    base = jax.random.randint(first_key, (N_ROWS, N_ROWS, TABLES), CAP // 3, 2 * CAP // 3 + 1)
    hottest = jax.random.randint(second_key, (TABLES,), 0, N_ROWS)
    is_hot = jnp.arange(N_ROWS)[None, :, None] == hottest[None, None, :]
    return jnp.where(is_hot, CAP, base).astype(jnp.int32)


def draw_slot_rows(key, part):
    first_key, second_key, third_key = jax.random.split(jax.random.fold_in(key, 23), 3)
    shape_all = (N_ROWS, N_ROWS, TABLES, CAP)
    first_draw = jax.random.randint(first_key, shape_all, 0, ROWS_DEV)
    second_draw = jax.random.randint(second_key, shape_all, 0, ROWS_DEV)
    offsets = jax.random.randint(third_key, (N_ROWS, TABLES), 0, ROWS_DEV)
    skewed = first_draw * second_draw // ROWS_DEV
    return ((skewed + offsets[None, :, :, None]) % ROWS_DEV).astype(jnp.int32)


def draw_slot_examples(key, part):
    first_key, second_key = jax.random.split(jax.random.fold_in(key, 37))
    shape_all = (N_ROWS, N_ROWS, TABLES, CAP)
    first_draw = jax.random.randint(first_key, shape_all, 0, B_DEV)
    second_draw = jax.random.randint(second_key, shape_all, 0, B_DEV)
    return jnp.minimum(first_draw, second_draw).astype(jnp.int32)


def shard_levels(key, dims, cuts, least, top_value):
    def one(axis_at, blocks):
        heights = jax.random.uniform(jax.random.fold_in(jax.random.fold_in(key, 6), axis_at), (blocks,), jnp.float32, least / len(cuts), top_value / len(cuts))
        return jnp.repeat(jnp.exp(heights), dims[axis_at] // blocks).reshape((-1,) + (1,) * (len(dims) - axis_at - 1))

    factor_of = one(*cuts[0])
    for cut in cuts[1:]:
        factor_of = factor_of * one(*cut)
    return factor_of


def bell_draw(rng, extent, width, most, cuts=(), kind=jnp.bfloat16):
    array = jax.random.normal(rng, extent, jnp.float32) * width
    if len(cuts) > 0:
        array = shard_levels(rng, extent, cuts, -0.22, 0.18) * array
    return jnp.clip(array, min=-most, max=most).astype(kind)


def setup_inputs(seed: int = 0) -> dict:
    keys = jax.random.split(jax.random.key(seed), 6)
    tables = bell_draw(keys[0], (TABLES, TABLE_ROWS, E), 0.25, 1.5, ((1, 64), (2, 4)), jnp.float32)
    dense_features = bell_draw(keys[1], (BATCH, E), 1.0, 6.0, ((0, 64), (1, 4)), jnp.float32)
    slot_rows = draw_slot_rows(jax.random.fold_in(keys[5], 71), 0)
    slot_examples = draw_slot_examples(jax.random.fold_in(keys[5], 71), 0)
    slot_counts = draw_slot_counts(jax.random.fold_in(keys[5], 71), 0)
    return {"tables": tables, "dense_features": dense_features, "slot_rows": slot_rows, "slot_examples": slot_examples, "slot_counts": slot_counts}


def reference(tables, dense_features, slot_rows, slot_examples, slot_counts):
    slot_index = jnp.arange(CAP, dtype=jnp.int32)
    live_slots = slot_index[None, None, None, :] < slot_counts[:, :, :, None]
    owner_base = (jnp.arange(N_ROWS, dtype=jnp.int32) * ROWS_DEV)[:, None, None]
    table_index = jnp.arange(TABLES, dtype=jnp.int32)[None, :, None]

    def one_source(pieces):
        rows_here, examples_here, live_here = pieces
        global_rows = (rows_here + owner_base).astype(jnp.int32)
        looked = tables[table_index, global_rows]
        looked = jnp.where(live_here[:, :, :, None], looked, jnp.zeros_like(looked))
        segment_ids = (examples_here * TABLES + table_index).astype(jnp.int32)
        summed = jax.ops.segment_sum(looked.reshape(-1, E), segment_ids.reshape(-1), num_segments=B_DEV * TABLES)
        return summed.reshape(B_DEV, TABLES, E)

    pooled = lax.map(one_source, (slot_rows, slot_examples, live_slots)).reshape(BATCH, TABLES, E)
    vectors = jnp.concatenate([dense_features[:, None, :], pooled], axis=1)
    gram_matrix = jnp.einsum("bie,bje->bij", vectors, vectors, precision=lax.Precision.HIGHEST)
    pair_first, pair_second = np.triu_indices(TABLES + 1, 1)
    interactions = gram_matrix[:, pair_first, pair_second] * (E ** -0.5)
    return pooled, interactions
```

```python
import functools

import jax
import jax.numpy as jnp
from jax import lax
from jax.experimental import pallas as pl
from jax.experimental.pallas import tpu as pltpu
from jax.sharding import PartitionSpec as P

E = 512
NX, NZ, NY = 4, 8, 4
TABLES = 4
ROWS_DEV = 512
B = 32
CAP = 64
W = 128
HALF_ROWS = 256
RA = 64
RB = TABLES * B - RA
N_SEM = 128
MESH = pl.DeviceIdType.MESH
F32 = jnp.float32
BF16 = jnp.bfloat16


def kernel(
    tables, dense, rows_in, ex_in, counts,
    pooled_out, inter_out,
    rows_v, ex_v, cnt_v, dense_v, tab_own, tab_oth, tb, msg, r1, r2, mb, part,
    xr, xl, xm, sa, zra, zla, zsra, zsla, zrb, zlb, zsrb, zslb, sb, bxr, bxl, bxm, fin,
    ybuf, yin, lsem, ssem, rsem,
):
    me = lax.axis_index("rows")
    y = lax.axis_index("cols")
    core = lax.rem(me, 2)
    chip = lax.div(me, 2)
    x = lax.rem(chip, NX)
    z = lax.div(chip, NX)

    def dev(dz=0, dx=0, dy=0, dc=0):
        zz = lax.rem(z + dz, NZ)
        xx = lax.rem(x + dx, NX)
        cc = lax.rem(core + dc, 2)
        return ((zz * NX + xx) * 2 + cc, lax.rem(y + dy, NY))

    used = []

    def send(src, dst, to):
        i = len(used)
        copy = pltpu.make_async_remote_copy(
            src_ref=src, dst_ref=dst, send_sem=ssem.at[i], recv_sem=rsem.at[i],
            device_id=to, device_id_type=MESH,
        )
        copy.start()
        used.append(copy)
        return copy

    locals_ = [
        pltpu.make_async_copy(rows_in, rows_v, lsem.at[0]),
        pltpu.make_async_copy(ex_in, ex_v, lsem.at[1]),
        pltpu.make_async_copy(counts, cnt_v, lsem.at[2]),
        pltpu.make_async_copy(tables, tab_own, lsem.at[3]),
        pltpu.make_async_copy(dense, dense_v, lsem.at[4]),
    ]
    for c in locals_:
        c.start()

    barrier = pltpu.get_barrier_semaphore()
    peers = [dev(dz=d) for d in range(1, NZ)] + [dev(dx=d) for d in range(1, NX)]
    peers += [dev(dy=d) for d in range(1, NY)] + [dev(dc=1)]
    for p in peers:
        pl.semaphore_signal(barrier, inc=1, device_id=p, device_id_type=MESH)

    for c in locals_[:3]:
        c.wait()
    lane = lax.broadcasted_iota(jnp.int32, (TABLES, W), 1)
    first = lane < CAP
    swap = core == 1
    for j in range(NX * NZ):
        own_r, oth_r = rows_v[j, core], rows_v[j, 1 - core]
        own_e, oth_e = ex_v[j, core], ex_v[j, 1 - core]
        even = jnp.broadcast_to(cnt_v[:, 2 * j : 2 * j + 1], (TABLES, W))
        odd = jnp.broadcast_to(cnt_v[:, 2 * j + 1 : 2 * j + 2], (TABLES, W))
        own_c = jnp.where(swap, odd, even)
        oth_c = jnp.where(swap, even, odd)
        bound = jnp.where(first, own_c, oth_c + CAP)
        ex = jnp.where(lane < bound, jnp.concatenate([own_e, oth_e], axis=1), -1)
        msg[j // NX, j % NX, 0:TABLES] = jnp.concatenate([own_r, oth_r], axis=1)
        msg[j // NX, j % NX, TABLES : 2 * TABLES] = ex

    pl.semaphore_wait(barrier, len(peers))

    ids_x = {}
    for j in (2, 1, 3):
        ids_x[j] = send(msg.at[:, lax.rem(x + j, NX)], r1.at[NX - j - 1], dev(dx=j))
    ids_z0 = {}
    for d in (4, 3, 5, 2, 6, 1, 7):
        ids_z0[d] = send(msg.at[lax.rem(z + d, NZ), x], r2.at[NZ - d, 0], dev(dz=d))
    tab_copy = send(tables, tab_oth, dev(dc=1))

    def split(src, half):
        for t in range(TABLES):
            v = src[t]
            hi = v.astype(BF16)
            lo = (v - hi.astype(F32)).astype(BF16)
            tb[t, half * ROWS_DEV : (half + 1) * ROWS_DEV, 0:W] = hi
            tb[t, half * ROWS_DEV : (half + 1) * ROWS_DEV, W : 2 * W] = lo

    locals_[3].wait()
    split(tab_own, 0)
    for j in (1, 2, 3):
        ids_x[j].wait_recv()
    ids_z1 = {}
    for d in (4, 3, 5, 2, 6, 1, 7):
        ids_z1[d] = send(r1.at[:, lax.rem(z + d, NZ)], r2.at[NZ - d, pl.ds(1, NX - 1)], dev(dz=d))
    tab_copy.wait_recv()
    split(tab_oth, 1)

    iota_a = lax.broadcasted_iota(jnp.int32, (W, W), 0)
    iota_b = lax.broadcasted_iota(jnp.int32, (HALF_ROWS, W), 0)
    core_key = jnp.where(first, 0, 2 * B)
    nt = (((1,), (1,)), ((), ()))

    def compute(zi):
        if zi:
            ids_z0[NZ - zi].wait_recv()
            ids_z1[NZ - zi].wait_recv()
        for s in range(NX):
            if zi:
                rows4, ex4 = r2[zi, s, 0:TABLES], r2[zi, s, TABLES : 2 * TABLES]
            elif s:
                rows4, ex4 = r1[s - 1, z, 0:TABLES], r1[s - 1, z, TABLES : 2 * TABLES]
            else:
                rows4, ex4 = msg[z, x, 0:TABLES], msg[z, x, TABLES : 2 * TABLES]
            key4 = jnp.where(ex4 >= 0, core_key + lax.shift_left(lax.shift_right_logical(rows4, 8), 5) + ex4, -1)
            low4 = rows4 & (HALF_ROWS - 1)
            for t in range(TABLES):
                a = jnp.where(iota_a == key4[t : t + 1], 1.0, 0.0).astype(BF16)
                b = jnp.where(iota_b == low4[t : t + 1], 1.0, 0.0).astype(BF16)
                m = lax.dot_general(a, b, nt, preferred_element_type=F32).astype(BF16)
                for q in range(4):
                    mb[t, s * B : (s + 1) * B, q * HALF_ROWS : (q + 1) * HALF_ROWS] = m[q * B : (q + 1) * B]
        for t in range(TABLES):
            o = jnp.dot(mb[t], tb[t], preferred_element_type=F32)
            o = o[:, 0:W] + o[:, W : 2 * W]
            for s in range(NX):
                part[zi, s, t * B : (t + 1) * B] = o[s * B : (s + 1) * B]

    class XPhase:
        def __init__(self, src, n, r, l, m):
            self.src, self.h, self.r, self.l, self.m = src, n // 2, r, l, m

        def piece(self, j, half):
            return self.src(j).at[pl.ds(half * self.h, self.h)]

        def start(self):
            self.r0 = send(self.piece(2, 0), self.r.at[0], dev(dx=1))
            self.l0 = send(self.piece(2, 1), self.l.at[0], dev(dx=NX - 1))
            self.r1 = send(self.piece(1, 1), self.r.at[1], dev(dx=1))
            self.l1 = send(self.piece(3, 0), self.l.at[1], dev(dx=NX - 1))

        def middle(self):
            self.r0.wait_recv()
            self.m[0] = self.r[0] + self.piece(1, 0)[...]
            self.r2 = send(self.m.at[0], self.r.at[2], dev(dx=1))
            self.l0.wait_recv()
            self.m[1] = self.l[0] + self.piece(3, 1)[...]
            self.l2 = send(self.m.at[1], self.l.at[2], dev(dx=NX - 1))

        def finish(self, out):
            for c in (self.r1, self.l1, self.r2, self.l2):
                c.wait_recv()
            out[0 : self.h] = self.piece(0, 0)[...] + self.l[1] + self.r[2]
            out[self.h : 2 * self.h] = self.piece(0, 1)[...] + self.r[1] + self.l[2]

    class ZPhase:
        def __init__(self, src, n, r, l, sr, sl):
            self.src, self.n, self.h = src, n, n // 2
            self.r, self.l, self.sr, self.sl = r, l, sr, sl
            self.cr, self.cl = {}, {}

        def step0(self):
            h = self.h
            self.cr[0] = send(self.src(4).at[pl.ds(0, h)], self.r(0).at[pl.ds(0, h)], dev(dz=1))
            self.cl[0] = send(self.src(4).at[pl.ds(h, h)], self.l(0).at[pl.ds(h, h)], dev(dz=NZ - 1))

        def step(self, k):
            h = self.h
            a, b = self.src(4 - k), self.src(4 + k)
            self.cr[k - 1].wait_recv()
            self.sr(k)[0:h] = self.r(k - 1)[0:h] + a[0:h]
            self.sr(k)[h:] = a[h:] if k == 1 else self.r(k - 1)[h:] + a[h:]
            self.cr[k] = send(self.sr(k), self.r(k), dev(dz=1))
            self.cl[k - 1].wait_recv()
            self.sl(k)[h:] = self.l(k - 1)[h:] + b[h:]
            self.sl(k)[0:h] = b[0:h] if k == 1 else self.l(k - 1)[0:h] + b[0:h]
            self.cl[k] = send(self.sl(k), self.l(k), dev(dz=NZ - 1))

        def finish(self, out):
            self.cr[3].wait_recv()
            self.cl[3].wait_recv()
            out[...] = self.src(0)[...] + self.r(3)[...] + self.l(3)[...]

    ax = [
        XPhase(lambda j, k=k: part.at[k, j, pl.ds(0, RA)], RA, xr.at[k], xl.at[k], xm.at[k])
        for k in range(NZ)
    ]
    az = ZPhase(
        lambda k: sa.at[k % NZ], RA, lambda k: zra.at[k], lambda k: zla.at[k],
        lambda k: zsra.at[k - 1], lambda k: zsla.at[k - 1],
    )
    bz = [
        ZPhase(
            lambda k, j=j: part.at[k % NZ, j, pl.ds(RA, RB)], RB,
            lambda k, j=j: zrb.at[k, j], lambda k, j=j: zlb.at[k, j],
            lambda k, j=j: zsrb.at[k - 1, j], lambda k, j=j: zslb.at[k - 1, j],
        )
        for j in range(NX)
    ]
    bx = XPhase(lambda j: sb.at[j], RB, bxr, bxl, bxm)
    order_j = (2, 1, 3, 0)

    def bstep(k):
        for j in order_j:
            bz[j].step(k)

    compute(0)
    ax[0].start()
    compute(4)
    for j in order_j:
        bz[j].step0()
    ax[4].start()
    ax[0].middle()
    compute(3)
    ax[3].start()
    compute(5)
    ax[5].start()
    ax[4].middle()
    ax[0].finish(sa.at[0])
    bstep(1)
    compute(2)
    ax[2].start()
    ax[3].middle()
    ax[5].middle()
    ax[4].finish(sa.at[4])
    az.step0()
    compute(6)
    ax[6].start()
    ax[2].middle()
    ax[3].finish(sa.at[3])
    ax[5].finish(sa.at[5])
    bstep(2)
    az.step(1)
    compute(1)
    ax[1].start()
    ax[6].middle()
    ax[2].finish(sa.at[2])
    compute(7)
    ax[7].start()
    ax[1].middle()
    ax[6].finish(sa.at[6])
    bstep(3)
    az.step(2)
    ax[7].middle()
    ax[1].finish(sa.at[1])
    ax[7].finish(sa.at[7])
    az.step(3)
    for j in order_j:
        bz[j].finish(sb.at[j])
    bx.start()
    bx.middle()
    az.finish(fin.at[pl.ds(0, RA)])
    bx.finish(fin.at[pl.ds(RA, RB)])

    locals_[4].wait()
    vec = [dense_v[...]] + [fin[t * B : (t + 1) * B] for t in range(TABLES)]
    for t in range(TABLES):
        pooled_out[:, t, :] = vec[1 + t]
    prods = [vec[i] * vec[j] for i in range(TABLES + 1) for j in range(i + 1, TABLES + 1)]
    prods += [jnp.zeros_like(prods[0])] * 2
    sums = []
    for g in range(3):
        stacked = jnp.concatenate(prods[4 * g : 4 * g + 4], axis=0)
        sums.append(jnp.sum(stacked.T, axis=0, keepdims=True))
    ybuf[...] = jnp.concatenate(sums + [jnp.zeros((5, W), F32)], axis=0)
    ycopies = [send(ybuf, yin.at[NY - j - 1], dev(dy=j)) for j in (2, 1, 3)]
    for c in ycopies:
        c.wait_recv()
    total = (ybuf[...] + yin[0] + yin[1] + yin[2]) * (E ** -0.5)
    for p in range(10):
        inter_out[p : p + 1, :] = total[p // 4 : p // 4 + 1, (p % 4) * B : (p % 4 + 1) * B]
    for c in used:
        c.wait_send()


def body(tables, dense, slot_rows, slot_examples, slot_counts):
    any_ = pl.BlockSpec(memory_space=pl.ANY)
    vmem = pl.BlockSpec(memory_space=pltpu.VMEM)
    V = pltpu.VMEM
    HA, HB = RA // 2, RB // 2
    scratch = [
        V((NX * NZ, 2, TABLES, CAP), jnp.int32),
        V((NX * NZ, 2, TABLES, CAP), jnp.int32),
        V((TABLES, 2 * NX * NZ), jnp.int32),
        V((B, W), F32),
        V((TABLES, ROWS_DEV, W), F32),
        V((TABLES, ROWS_DEV, W), F32),
        V((TABLES, 2 * ROWS_DEV, 2 * W), BF16),
        V((NZ, NX, 8, W), jnp.int32),
        V((NX - 1, NZ, 8, W), jnp.int32),
        V((NZ, NX, 8, W), jnp.int32),
        V((TABLES, W, 4 * HALF_ROWS), BF16),
        V((NZ, NX, TABLES * B, W), F32),
        V((NZ, 3, HA, W), F32),
        V((NZ, 3, HA, W), F32),
        V((NZ, 2, HA, W), F32),
        V((NZ, RA, W), F32),
        V((4, RA, W), F32),
        V((4, RA, W), F32),
        V((3, RA, W), F32),
        V((3, RA, W), F32),
        V((4, NX, RB, W), F32),
        V((4, NX, RB, W), F32),
        V((3, NX, RB, W), F32),
        V((3, NX, RB, W), F32),
        V((NX, RB, W), F32),
        V((3, HB, W), F32),
        V((3, HB, W), F32),
        V((2, HB, W), F32),
        V((TABLES * B, W), F32),
        V((8, W), F32),
        V((NY - 1, 8, W), F32),
        pltpu.SemaphoreType.DMA((5,)),
        pltpu.SemaphoreType.DMA((N_SEM,)),
        pltpu.SemaphoreType.DMA((N_SEM,)),
    ]
    pooled, inter = pl.pallas_call(
        kernel,
        out_shape=(
            jax.ShapeDtypeStruct((B, TABLES, W), F32),
            jax.ShapeDtypeStruct((10, B), F32),
        ),
        in_specs=[any_] * 5,
        out_specs=(vmem, vmem),
        scratch_shapes=scratch,
        compiler_params=pltpu.CompilerParams(
            collective_id=0, has_side_effects=True, vmem_limit_bytes=56 * 1024 * 1024
        ),
    )(
        tables,
        dense,
        slot_rows.reshape(NX * NZ, 2, TABLES, CAP),
        slot_examples.reshape(NX * NZ, 2, TABLES, CAP),
        slot_counts[0].T,
    )
    return pooled, inter.T


def solution(mesh):
    return jax.shard_map(
        body,
        mesh=mesh,
        in_specs=(
            P(None, "rows", "cols"),
            P("rows", "cols"),
            P("rows", None, None, None),
            P("rows", None, None, None),
            P("rows", None, None),
        ),
        out_specs=(P("rows", None, "cols"), P("rows", None)),
        check_vma=False,
    )
```
